32 devices in a mesh: dp: 8 (over z, core), expert: 4 (over y, x).
Axes of the slice: x: 2, y: 2, z: 4, core: 2. Of those that a mesh axis runs over, the one named last changes fastest.
Arguments:
- tokens: bfloat16 [2048, 4, 1536], P('dp', 'expert'), may hold values from -6 to 6
- route_ids: int32 [4, 2048, 2], P('expert', 'dp'), may hold values from 0 to 7, all different within a row; in each aligned block of 256 rows (0 to 255, 256 to 511, ..., all dimensions but the last counted through in order) at most 96 rows name the same one
- router: bfloat16 [4, 1536, 8], P('expert'), may hold values from -0.15625 to 0.15625
- norm_gain: float32 [4, 1536], P('expert'), may hold values from 0.5 to 1.5
- w_in: bfloat16 [4, 8, 1536, 768], P('expert', 'dp'), may hold values from -0.15625 to 0.15625
- w_out: bfloat16 [4, 8, 768, 1536], P('expert', 'dp'), may hold values from -0.21875 to 0.21875
- cotangent: bfloat16 [2048, 4, 1536], P('dp', 'expert'), may hold values from -6 to 6
Outputs:
- normed_out: bfloat16 [2048, 4, 1536], P('dp', 'expert')
- grad_tokens: bfloat16 [2048, 4, 1536], P('dp', 'expert')
- grad_router: float32 [4, 1536, 8], P('expert')
- grad_gain: float32 [4, 1536], P('expert')
- grad_w_in: bfloat16 [4, 8, 1536, 768], P('expert', 'dp')
- grad_w_out: bfloat16 [4, 8, 768, 1536], P('expert', 'dp')
The draws below stay inside these ranges and needn't reach their ends.
Inputs may be any that keep to these rules, and one draw needn't show every extreme that they name: `route_ids`: the two ids of a row differ. Among the rows of one device (one mixed token, 256 samples, two choices each) no expert is named more than 96 times.
All inputs are finite; a program needn't handle non-finite values.
Results may differ from the reference program's by a relative error of at most 0.015.
Values may be sent and summed in bfloat16 or wider, within the bound.
No kernel may reach another device: no remote copies, remote signals or barrier semaphores. Data moves between devices by JAX's collectives and lax.ppermute only.
A program may use at most 64 MiB of HBM per device.

```python
import math
import jax
import jax.numpy as jnp
import numpy as np
from jax import lax

D = 1536
HID = 768
TOP = 2
SAMP_DEV = 256
FEAT = 4
EXPERTS = 8
CAP = 96
SAMPLES = 2048
N_DP = 8


def block_levels(key, dims, shards, smallest, largest):
    loudness, own = 1.0, jax.random.fold_in(key, 6)
    for axis_at, parts in shards:
        steps = jnp.exp(jax.random.uniform(jax.random.fold_in(own, axis_at), (parts,), jnp.float32, smallest / len(shards), largest / len(shards)))
        loudness = loudness * jnp.repeat(steps, dims[axis_at] // parts).reshape([-1 if axis == axis_at else 1 for axis in range(len(dims))])
    return loudness


def shared_out(own_key, own, number, rows, number_of, top, limit, skew):
    sequence = jax.random.permutation(own_key, number_of)
    packed, ordinary = portions_of(number_of, rows * top, limit, skew, True), portions_of(number_of, rows * top, limit, skew, False)
    places = jnp.arange(number_of)

    def named(tallies, offset_by):
        used = int((tallies > 0).sum())
        fixed = max(1, used // 4)
        moved = fixed + (places - fixed + offset_by * (used - fixed)) % max(1, number_of - fixed)
        return jnp.zeros((number_of,), jnp.int32).at[sequence[jnp.where(places < fixed, places, moved)]].set(jnp.asarray(tallies, jnp.int32))

    tallies = jnp.where(number % 4 == 0, named(packed, number // 4), named(ordinary, number - number // 4 - 1))
    mixed = jax.random.permutation(jax.random.fold_in(own, 3), number_of)
    source_of, sink = mixed[0:number_of // 2 * 2:2], mixed[1:number_of // 2 * 2:2]
    margin = jnp.minimum(tallies[source_of] - 1, limit - tallies[sink]) // 2
    margin = jnp.where((source_of == sequence[0]) | (sink == sequence[0]) | (tallies[sink] == 0), 0, jnp.maximum(margin, 0))
    moved = jax.random.randint(jax.random.fold_in(own, 4), (number_of // 2,), 0, 1 << 20) % (margin + 1)
    tallies = tallies.at[source_of].add(-moved).at[sink].add(moved)
    items = jnp.searchsorted(jnp.cumsum(tallies), jnp.arange(rows * top), side="right").astype(jnp.int32)
    grid = items.reshape(top, rows).T
    grid = grid[jax.random.permutation(jax.random.fold_in(own, 1), rows)]
    offset_by = jax.random.randint(jax.random.fold_in(own, 2), (rows, 1), 0, top)
    return jnp.take_along_axis(grid, (jnp.arange(top)[None, :] + offset_by) % top, axis=1)


def portions_of(number_of, total, bound, slope, full):
    weights = [(1 << 20) // math.isqrt(grade ** slope) + 1 for grade in range(1, number_of + 1)]
    largest = bound if full else min(bound, max(-(-total // number_of), total * weights[0] // sum(weights)))
    least = 1 if total - largest >= number_of - 1 else 0
    counts, rest = [largest] + [least] * (number_of - 1), total - largest - least * (number_of - 1)
    while rest > 0:
        candidates = [i for i in range(1, number_of) if counts[i] < largest] or [i for i in range(1, number_of) if counts[i] < bound]
        pool, remaining = sum([weights[i] for i in candidates]), rest
        for i in candidates:
            addition = min(bound - counts[i], max(1, remaining * weights[i] // pool), rest)
            counts[i] = counts[i] + addition
            rest = rest - addition
    return np.array(counts)


def scatter_about(key, dims, scale, limit, cuts=(), kind=jnp.bfloat16):
    array = jax.random.normal(key, dims, jnp.float32) * scale
    if len(cuts) > 0:
        array = block_levels(key, dims, cuts, -0.22, 0.18) * array
    return jnp.clip(array, min=-limit, max=limit).astype(kind)


def setup_inputs(seed: int = 0) -> dict:
    streams_of = jax.random.split(jax.random.key(seed), 8)
    tokens = scatter_about(streams_of[0], (SAMPLES, FEAT, D), 1.0, 6.0, ((0, 8), (1, 4)))
    route_ids_keys = jax.random.split(jax.random.fold_in(streams_of[1], 1), FEAT * SAMPLES // SAMP_DEV)
    route_ids_turns = jax.random.permutation(jax.random.fold_in(streams_of[1], 3), FEAT * SAMPLES // SAMP_DEV)
    route_ids = jax.vmap(lambda own, number: shared_out(jax.random.fold_in(streams_of[1], 2), own, number, SAMP_DEV, EXPERTS, 2, CAP, 2))(route_ids_keys, route_ids_turns).reshape((FEAT, SAMPLES, TOP))
    router = scatter_about(streams_of[2], (FEAT, D, EXPERTS), D ** -0.5, 0.15625, ((0, 4),))
    norm_gain = jnp.clip(1.0 + 0.1 * jax.random.normal(streams_of[3], (FEAT, D), jnp.float32), 0.5, 1.5)
    w_in = scatter_about(streams_of[4], (FEAT, EXPERTS, D, HID), D ** -0.5, 0.15625, ((0, 4), (1, 8)))
    w_out = scatter_about(streams_of[5], (FEAT, EXPERTS, HID, D), HID ** -0.5, 0.21875, ((0, 4), (1, 8)))
    cotangent = scatter_about(streams_of[6], (SAMPLES, FEAT, D), 1.0, 6.0, ((0, 8), (1, 4)))
    return {"tokens": tokens, "route_ids": route_ids, "router": router, "norm_gain": norm_gain, "w_in": w_in, "w_out": w_out, "cotangent": cotangent}


gelu_coef = 0.7978845608028654
cubic_coef = 0.044715
norm_eps = 1e-05

def gelu_tanh(value):
    inner = gelu_coef * (value + cubic_coef * value * value * value)
    return 0.5 * value * (1.0 + jnp.tanh(inner))

def gelu_slope(value):
    inner = gelu_coef * (value + cubic_coef * value * value * value)
    tangent = jnp.tanh(inner)
    return 0.5 * (1.0 + tangent) + 0.5 * value * (1.0 - tangent * tangent) * gelu_coef * (1.0 + 3.0 * cubic_coef * value * value)

def swap_heads(values):
    samples, token_count, model_width = values.shape
    head_size = model_width // token_count
    return values.reshape(samples, token_count, token_count, head_size).transpose(0, 2, 1, 3).reshape(samples, token_count, model_width)

def one_token(inputs):
    mixed_rows, route_rows, router_row, gain_row, weight_in, weight_out, cot_rows = inputs
    samples = mixed_rows.shape[0]
    model_width = mixed_rows.shape[1]
    experts = weight_in.shape[0]
    slot_rows = N_DP * CAP
    labels = jnp.arange(experts, dtype=jnp.int32)
    chosen = (route_rows[:, :, None] == labels[None, None, :]).astype(jnp.int32)
    flat_hot = chosen.reshape(samples * 2, experts)
    before = jnp.cumsum(flat_hot, axis=0, dtype=jnp.int32) - flat_hot
    slot_place = lax.optimization_barrier(jnp.sum(before * flat_hot, axis=1, dtype=jnp.int32)).reshape(samples, 2)
    chosen_f = chosen.astype(jnp.float32)
    logits = jnp.dot(mixed_rows, router_row, preferred_element_type=jnp.float32)
    picked = lax.optimization_barrier(jnp.sum(logits[:, None, :] * chosen_f, axis=2))
    gate_value = jax.nn.sigmoid(picked)
    doubled = jnp.broadcast_to(mixed_rows[:, None, :], (samples, 2, model_width))
    buffer = jnp.zeros((experts, slot_rows, model_width), jnp.bfloat16).at[route_rows, slot_place].set(doubled)
    pre_act = jnp.einsum('erd,edh->erh', buffer.astype(jnp.float32), weight_in.astype(jnp.float32))
    act_values = gelu_tanh(pre_act).astype(jnp.bfloat16)
    result = jnp.einsum('erh,ehd->erd', act_values.astype(jnp.float32), weight_out.astype(jnp.float32)).astype(jnp.bfloat16)
    routed_f = result[route_rows, slot_place].astype(jnp.float32)
    expert_sum = gate_value[:, 0:1] * routed_f[:, 0] + gate_value[:, 1:2] * routed_f[:, 1]
    residual = mixed_rows.astype(jnp.float32) + expert_sum
    row_mean = lax.optimization_barrier(jnp.mean(residual, axis=1, keepdims=True))
    centered = residual - row_mean
    row_var = lax.optimization_barrier(jnp.mean(centered * centered, axis=1, keepdims=True))
    inv_std = lax.rsqrt(row_var + norm_eps)
    normed = centered * inv_std
    normed_out = (normed * gain_row[None, :]).astype(jnp.bfloat16)
    cot_f = cot_rows.astype(jnp.float32)
    grad_gain = lax.optimization_barrier(jnp.sum(cot_f * normed, axis=0))
    grad_normed = cot_f * gain_row[None, :]
    grad_resid = inv_std * (grad_normed - lax.optimization_barrier(jnp.mean(grad_normed, axis=1, keepdims=True)) - normed * lax.optimization_barrier(jnp.mean(grad_normed * normed, axis=1, keepdims=True)))
    grad_rounded = lax.optimization_barrier(grad_resid.astype(jnp.bfloat16)).astype(jnp.float32)
    grad_exp_out = (gate_value[:, :, None] * grad_rounded[:, None, :]).astype(jnp.bfloat16)
    grad_buffer = jnp.zeros((experts, slot_rows, model_width), jnp.bfloat16).at[route_rows, slot_place].set(grad_exp_out)
    grad_gate = lax.optimization_barrier(jnp.sum(grad_resid[:, None, :] * routed_f, axis=2))
    grad_logit = grad_gate * gate_value * (1.0 - gate_value)
    route_grad = lax.optimization_barrier(jnp.sum(grad_logit[:, :, None] * chosen_f, axis=1))
    grad_buffer_f = grad_buffer.astype(jnp.float32)
    grad_act = jnp.einsum('erd,ehd->erh', grad_buffer_f, weight_out.astype(jnp.float32))
    grad_pre = (grad_act * gelu_slope(pre_act)).astype(jnp.bfloat16)
    grad_w_out = jnp.einsum('erh,erd->ehd', act_values.astype(jnp.float32), grad_buffer_f).astype(jnp.bfloat16)
    grad_w_in = jnp.einsum('erd,erh->edh', buffer.astype(jnp.float32), grad_pre.astype(jnp.float32)).astype(jnp.bfloat16)
    grad_input = jnp.einsum('erh,edh->erd', grad_pre.astype(jnp.float32), weight_in.astype(jnp.float32)).astype(jnp.bfloat16)
    grad_routed = grad_input[route_rows, slot_place].astype(jnp.float32)
    router_f = router_row.astype(jnp.float32)
    grad_mixed = grad_resid + grad_routed[:, 0] + grad_routed[:, 1] + jnp.dot(route_grad, router_f.T, precision=lax.Precision.HIGHEST)
    grad_router = jnp.dot(mixed_rows.astype(jnp.float32).T, route_grad, precision=lax.Precision.HIGHEST)
    return (normed_out, grad_mixed.astype(jnp.bfloat16), grad_router, grad_gain, grad_w_in, grad_w_out)

def reference(tokens, route_ids, router, norm_gain, w_in, w_out, cotangent):
    mixed_all = swap_heads(tokens).transpose(1, 0, 2)
    cot_all = cotangent.transpose(1, 0, 2)
    normed_out, grad_mixed, grad_router, grad_gain, grad_w_in, grad_w_out = lax.map(one_token, (mixed_all, route_ids, router, norm_gain, w_in, w_out, cot_all))
    normed_out = normed_out.transpose(1, 0, 2)
    grad_tokens = swap_heads(grad_mixed.transpose(1, 0, 2))
    return (normed_out, grad_tokens, grad_router, grad_gain, grad_w_in, grad_w_out)
```

```python
import jax
import jax.numpy as jnp
from jax import lax
from jax.sharding import PartitionSpec as P

gelu_coef = 0.7978845608028654
cubic_coef = 0.044715
norm_eps = 1e-05
CHUNKS = 2


def gelu_tanh(value):
    inner = gelu_coef * (value + cubic_coef * value * value * value)
    return 0.5 * value * (1.0 + jnp.tanh(inner))


def gelu_slope(value):
    inner = gelu_coef * (value + cubic_coef * value * value * value)
    tangent = jnp.tanh(inner)
    return 0.5 * (1.0 + tangent) + 0.5 * value * (1.0 - tangent * tangent) * gelu_coef * (
        1.0 + 3.0 * cubic_coef * value * value
    )


def exchange(blocks):
    return lax.all_to_all(blocks, "dp", split_axis=0, concat_axis=0, tiled=True)


def dot(a, b, dims):
    return lax.dot_general(a, b, (dims, ((), ())), preferred_element_type=jnp.float32)


def body(tokens, route_ids, router, norm_gain, w_in, w_out, cotangent):
    row_count = tokens.shape[0]
    model_width = tokens.shape[2]
    experts = lax.axis_size("dp")
    slot_depth = 3 * row_count // experts
    part = slot_depth // CHUNKS
    part_rows = experts * part
    weight_in = w_in[0, 0]
    weight_out = w_out[0, 0]
    hidden = weight_in.shape[1]
    router_row = router[0]
    gain_row = norm_gain[0]
    me = lax.axis_index("dp")
    own_rows = tokens.reshape(row_count, model_width)
    mixed_rows = lax.all_to_all(own_rows, "expert", split_axis=1, concat_axis=1, tiled=True)
    route_rows = route_ids.reshape(row_count, 2)
    labels = lax.broadcasted_iota(jnp.int32, (row_count, 2, experts), 2)
    chosen = (route_rows[:, :, None] == labels).astype(jnp.int32)
    flat_hot = chosen.reshape(row_count * 2, experts)
    before = jnp.cumsum(flat_hot, axis=0, dtype=jnp.int32) - flat_hot
    slot_place = jnp.sum(before * flat_hot, axis=1, dtype=jnp.int32).reshape(row_count, 2)
    chunk_of = slot_place // part
    target = route_rows * part + slot_place - chunk_of * part
    slot_index = lax.broadcasted_iota(jnp.int32, (part_rows, row_count), 0)
    placers = []
    for c in range(CHUNKS):
        here = jnp.where(chunk_of == c, target, -1)
        placers.append(
            jnp.logical_or(here[None, :, 0] == slot_index, here[None, :, 1] == slot_index).astype(
                jnp.bfloat16
            )
        )
    my_column = lax.broadcasted_iota(jnp.int32, (1, experts), 1) == me

    def spread(placer, rows):
        picked = dot(placer, rows, ((1,), (0,))).astype(jnp.bfloat16)
        return picked.reshape(experts, part, model_width)

    arrived = [exchange(spread(p, mixed_rows)).reshape(part_rows, model_width) for p in placers]
    saved = []
    expert_sum = mixed_rows.astype(jnp.float32)
    for c in range(CHUNKS):
        rows = arrived[c]
        logits = dot(rows, router_row, ((1,), (0,)))
        gate = jax.nn.sigmoid(jnp.sum(jnp.where(my_column, logits, 0.0), axis=1, keepdims=True))
        pre_act = dot(rows, weight_in, ((1,), (0,)))
        act = gelu_tanh(pre_act).astype(jnp.bfloat16)
        out = dot(act, weight_out, ((1,), (0,)))
        result = out.astype(jnp.bfloat16)
        gated = (gate * out).astype(jnp.bfloat16)
        saved.append((rows, gate, pre_act, act, result))
        returned = exchange(gated.reshape(experts, part, model_width))
        expert_sum = expert_sum + dot(
            placers[c], returned.reshape(part_rows, model_width), ((0,), (0,))
        )
    residual = expert_sum
    row_mean = jnp.mean(residual, axis=1, keepdims=True)
    centered = residual - row_mean
    row_var = jnp.mean(centered * centered, axis=1, keepdims=True)
    inv_std = lax.rsqrt(row_var + norm_eps)
    normed = centered * inv_std
    normed_out = (normed * gain_row[None, :]).astype(jnp.bfloat16)
    cot_f = cotangent.reshape(row_count, model_width).astype(jnp.float32)
    grad_gain = jnp.sum(cot_f * normed, axis=0)
    grad_normed = cot_f * gain_row[None, :]
    grad_resid = inv_std * (
        grad_normed
        - jnp.mean(grad_normed, axis=1, keepdims=True)
        - normed * jnp.mean(grad_normed * normed, axis=1, keepdims=True)
    )
    grad_rounded = grad_resid.astype(jnp.bfloat16)

    grad_arrived = [exchange(spread(p, grad_rounded)).reshape(part_rows, model_width) for p in placers]
    router_mine = jnp.sum(jnp.where(my_column, router_row.astype(jnp.float32), 0.0), axis=1)
    grad_mixed = grad_resid
    pre_grads, out_grads, logit_grads = [], [], []
    for c in range(CHUNKS):
        rows, gate, pre_act, act, result = saved[c]
        grads = grad_arrived[c].astype(jnp.float32)
        grad_out = (gate * grads).astype(jnp.bfloat16)
        grad_gate = jnp.sum(grads * result.astype(jnp.float32), axis=1, keepdims=True)
        grad_logit = grad_gate * gate * (1.0 - gate)
        grad_act = dot(grad_out, weight_out, ((1,), (1,)))
        grad_pre = (grad_act * gelu_slope(pre_act)).astype(jnp.bfloat16)
        grad_input = dot(grad_pre, weight_in, ((1,), (1,))) + grad_logit * router_mine[None, :]
        back = exchange(grad_input.astype(jnp.bfloat16).reshape(experts, part, model_width))
        grad_mixed = grad_mixed + dot(placers[c], back.reshape(part_rows, model_width), ((0,), (0,)))
        pre_grads.append(grad_pre)
        out_grads.append(grad_out)
        logit_grads.append(grad_logit)
    all_rows = jnp.concatenate([s[0] for s in saved])
    all_act = jnp.concatenate([s[3] for s in saved])
    all_logit = jnp.concatenate(logit_grads)
    router_part = jnp.sum(all_rows.astype(jnp.float32) * all_logit, axis=0)
    lanes = 128
    small = jnp.stack([router_part, grad_gain]).reshape(1, 2 * model_width // lanes, lanes)
    small = exchange(jnp.broadcast_to(small, (experts,) + small.shape[1:]))
    small = small.reshape(experts, 2, model_width)
    grad_router = small[:, 0].T
    grad_gain_sum = jnp.sum(small[:, 1], axis=0)
    grad_w_out = dot(all_act, jnp.concatenate(out_grads), ((0,), (0,))).astype(jnp.bfloat16)
    grad_w_in = dot(all_rows, jnp.concatenate(pre_grads), ((0,), (0,))).astype(jnp.bfloat16)
    grad_tokens = lax.all_to_all(
        grad_mixed.astype(jnp.bfloat16), "expert", split_axis=1, concat_axis=1, tiled=True
    )
    return (
        normed_out.reshape(row_count, 1, model_width),
        grad_tokens.reshape(row_count, 1, model_width),
        grad_router.reshape(1, model_width, experts),
        grad_gain_sum.reshape(1, model_width),
        grad_w_in.reshape(1, 1, model_width, hidden),
        grad_w_out.reshape(1, 1, hidden, model_width),
    )


def solution(mesh):
    return jax.shard_map(
        body,
        mesh=mesh,
        in_specs=(
            P("dp", "expert", None),
            P("expert", "dp", None),
            P("expert", None, None),
            P("expert", None),
            P("expert", "dp", None, None),
            P("expert", "dp", None, None),
            P("dp", "expert", None),
        ),
        out_specs=(
            P("dp", "expert", None),
            P("dp", "expert", None),
            P("expert", None, None),
            P("expert", None),
            P("expert", "dp", None, None),
            P("expert", "dp", None, None),
        ),
        check_vma=False,
    )
```

```python
import jax
import jax.numpy as jnp
from jax import lax
from jax.sharding import PartitionSpec as P


gelu_coef = 0.7978845608028654
cubic_coef = 0.044715
norm_eps = 1e-05


def gelu_tanh(value):
    inner = gelu_coef * (value + cubic_coef * value * value * value)
    return 0.5 * value * (1.0 + jnp.tanh(inner))


def gelu_slope(value):
    inner = gelu_coef * (value + cubic_coef * value * value * value)
    tangent = jnp.tanh(inner)
    return 0.5 * (1.0 + tangent) + 0.5 * value * (1.0 - tangent * tangent) * gelu_coef * (
        1.0 + 3.0 * cubic_coef * value * value
    )


def dot(a, b, dims):
    return lax.dot_general(a, b, (dims, ((), ())), preferred_element_type=jnp.float32)


def xor_pairs(size, k):
    return [(i, i ^ k) for i in range(size)]


def swap_cores(rows):
    return lax.ppermute(rows, "dp", xor_pairs(lax.axis_size("dp"), 1))


def to_chip(rows, k):
    return lax.ppermute(rows, "dp", xor_pairs(lax.axis_size("dp"), 2 * k)) if k else rows


def exchange(blocks):
    return lax.all_to_all(blocks, "dp", split_axis=0, concat_axis=0, tiled=True)


def mix_heads(rows):
    count = lax.axis_size("expert")
    mine = lax.axis_index("expert")
    head = rows.shape[1] // count
    if head % 128 or count & (count - 1):
        return lax.all_to_all(rows, "expert", split_axis=1, concat_axis=1, tiled=True)
    pieces = []
    for k in range(count):
        piece = lax.dynamic_slice_in_dim(rows, (mine ^ k) * head, head, 1)
        pieces.append(lax.ppermute(piece, "expert", xor_pairs(count, k)) if k else piece)
    stacked = jnp.stack(pieces)
    return jnp.concatenate(
        [lax.dynamic_index_in_dim(stacked, mine ^ t, 0, False) for t in range(count)], axis=1
    )


def body(tokens, route_ids, router, norm_gain, w_in, w_out, cotangent):
    row_count = tokens.shape[0]
    model_width = tokens.shape[2]
    experts = lax.axis_size("dp")
    chips = experts // 2
    depth = 3 * row_count // experts
    weight_in = w_in[0, 0]
    weight_out = w_out[0, 0]
    hidden = weight_in.shape[1]
    router_row = router[0]
    gain_row = norm_gain[0]
    me = lax.axis_index("dp")
    far = list(range(chips // 2, chips))
    near = list(range(chips // 2))
    groups = [far[:1], near] + [[k] for k in far[1:]]

    route_rows = route_ids.reshape(row_count, 2)
    labels = lax.broadcasted_iota(jnp.int32, (row_count, 2, experts), 2)
    flat_hot = (route_rows[:, :, None] == labels).astype(jnp.int32).reshape(row_count * 2, experts)
    before = jnp.cumsum(flat_hot, axis=0, dtype=jnp.int32) - flat_hot
    slot_place = jnp.sum(before * flat_hot, axis=1, dtype=jnp.int32).reshape(row_count, 2)
    target = (route_rows ^ me) * depth + slot_place

    def placer_of(group):
        rows = []
        for k in group:
            slot = lax.broadcasted_iota(jnp.int32, (2 * depth, row_count), 0) + 2 * k * depth
            rows.append(jnp.logical_or(target[None, :, 0] == slot, target[None, :, 1] == slot))
        return jnp.concatenate(rows).astype(jnp.bfloat16) if len(rows) > 1 else rows[0].astype(jnp.bfloat16)

    placers = [placer_of(g) for g in groups]
    my_column = lax.broadcasted_iota(jnp.int32, (1, experts), 1) == me
    router_mine = jnp.sum(jnp.where(my_column, router_row.astype(jnp.float32), 0.0), axis=1)

    def dispatch(rows):
        arrived = []
        for group, placer in zip(groups, placers):
            slots = dot(placer, rows, ((1,), (0,))).astype(jnp.bfloat16)
            parts = [to_chip(slots[2 * depth * i : 2 * depth * (i + 1)], k) for i, k in enumerate(group)]
            mine = jnp.concatenate([p[:depth] for p in parts])
            others = jnp.concatenate([p[depth:] for p in parts])
            arrived.append(jnp.concatenate([mine, swap_cores(others)]))
        return arrived

    def give_back(group, rows):
        half = len(group) * depth
        others = swap_cores(rows[half:])
        parts = []
        for i, k in enumerate(group):
            pair = jnp.concatenate([rows[depth * i : depth * (i + 1)], others[depth * i : depth * (i + 1)]])
            parts.append(to_chip(pair, k))
        return jnp.concatenate(parts)

    def collect(parts):
        return sum(dot(p, r, ((0,), (0,))) for p, r in zip(placers, parts))

    mixed = mix_heads(tokens.reshape(row_count, model_width))
    kept, parts = [], []
    for group, rows in zip(groups, dispatch(mixed)):
        logits = lax.optimization_barrier(dot(rows, router_row, ((1,), (0,))))
        gate = jax.nn.sigmoid(jnp.sum(jnp.where(my_column, logits, 0.0), axis=1, keepdims=True))
        pre_act = dot(rows, weight_in, ((1,), (0,)))
        act = gelu_tanh(pre_act).astype(jnp.bfloat16)
        out = dot(act, weight_out, ((1,), (0,)))
        kept.append((rows, gate, pre_act, act, out.astype(jnp.bfloat16)))
        parts.append(give_back(group, (gate * out).astype(jnp.bfloat16)))
    residual = mixed.astype(jnp.float32) + collect(parts)
    row_mean = jnp.mean(residual, axis=1, keepdims=True)
    centered = residual - row_mean
    row_var = jnp.mean(centered * centered, axis=1, keepdims=True)
    inv_std = lax.rsqrt(row_var + norm_eps)
    normed = centered * inv_std
    normed_out = (normed * gain_row[None, :]).astype(jnp.bfloat16)
    cot_f = cotangent.reshape(row_count, model_width).astype(jnp.float32)
    grad_gain = jnp.sum(cot_f * normed, axis=0)
    grad_normed = cot_f * gain_row[None, :]
    grad_resid = inv_std * (
        grad_normed
        - jnp.mean(grad_normed, axis=1, keepdims=True)
        - normed * jnp.mean(grad_normed * normed, axis=1, keepdims=True)
    )

    slopes = lax.optimization_barrier([gelu_slope(s[2]) for s in kept])
    parts, pre_grads, out_grads, logit_grads = [], [], [], []
    arrived = dispatch(grad_resid.astype(jnp.bfloat16))
    for g, (group, grads, saved) in enumerate(zip(groups, arrived, kept)):
        rows, gate, pre_act, act, result = saved
        grads_f = grads.astype(jnp.float32)
        grad_out = (gate * grads_f).astype(jnp.bfloat16)
        grad_gate = jnp.sum(grads_f * result.astype(jnp.float32), axis=1, keepdims=True)
        grad_logit = grad_gate * gate * (1.0 - gate)
        grad_act = dot(grad_out, weight_out, ((1,), (1,)))
        grad_pre = (grad_act * slopes[g]).astype(jnp.bfloat16)
        grad_input = dot(grad_pre, weight_in, ((1,), (1,))) + grad_logit * router_mine[None, :]
        parts.append(give_back(group, grad_input.astype(jnp.bfloat16)))
        pre_grads.append(grad_pre)
        out_grads.append(grad_out)
        logit_grads.append(grad_logit)
    grad_mixed = grad_resid + collect(parts)
    grad_tokens = mix_heads(grad_mixed.astype(jnp.bfloat16))

    all_rows = jnp.concatenate([s[0] for s in kept])
    all_act = jnp.concatenate([s[3] for s in kept])
    router_part = jnp.sum(all_rows.astype(jnp.float32) * jnp.concatenate(logit_grads), axis=0)
    lanes = 128
    small = jnp.stack([router_part, grad_gain]).reshape(1, 2 * model_width // lanes, lanes)
    small = exchange(jnp.broadcast_to(small, (experts,) + small.shape[1:]))
    small = small.reshape(experts, 2, model_width)
    grad_w_out = dot(all_act, jnp.concatenate(out_grads), ((0,), (0,))).astype(jnp.bfloat16)
    grad_w_in = dot(all_rows, jnp.concatenate(pre_grads), ((0,), (0,))).astype(jnp.bfloat16)
    return (
        normed_out.reshape(row_count, 1, model_width),
        grad_tokens.reshape(row_count, 1, model_width),
        small[:, 0].T.reshape(1, model_width, experts),
        jnp.sum(small[:, 1], axis=0).reshape(1, model_width),
        grad_w_in.reshape(1, 1, model_width, hidden),
        grad_w_out.reshape(1, 1, hidden, model_width),
    )


def solution(mesh):
    return jax.shard_map(
        body,
        mesh=mesh,
        in_specs=(
            P("dp", "expert", None),
            P("expert", "dp", None),
            P("expert", None, None),
            P("expert", None),
            P("expert", "dp", None, None),
            P("expert", "dp", None, None),
            P("dp", "expert", None),
        ),
        out_specs=(
            P("dp", "expert", None),
            P("dp", "expert", None),
            P("expert", None, None),
            P("expert", None),
            P("expert", "dp", None, None),
            P("expert", "dp", None, None),
        ),
        check_vma=False,
    )
```

```python
import jax
import jax.numpy as jnp
from jax import lax
from jax.sharding import PartitionSpec as P


gelu_coef = 0.7978845608028654
cubic_coef = 0.044715
norm_eps = 1e-05


def gelu_tanh(value):
    inner = gelu_coef * (value + cubic_coef * value * value * value)
    return 0.5 * value * (1.0 + jnp.tanh(inner))


def gelu_slope(value):
    inner = gelu_coef * (value + cubic_coef * value * value * value)
    tangent = jnp.tanh(inner)
    return 0.5 * (1.0 + tangent) + 0.5 * value * (1.0 - tangent * tangent) * gelu_coef * (
        1.0 + 3.0 * cubic_coef * value * value
    )


def dot(a, b, dims):
    return lax.dot_general(a, b, (dims, ((), ())), preferred_element_type=jnp.float32)


def after(rows, *others):
    return lax.optimization_barrier((rows,) + others)[0]


def xor_pairs(size, k):
    return [(i, i ^ k) for i in range(size)]


def swap_cores(rows):
    return lax.ppermute(rows, "dp", xor_pairs(lax.axis_size("dp"), 1))


def to_chip(rows, k):
    return lax.ppermute(rows, "dp", xor_pairs(lax.axis_size("dp"), 2 * k)) if k else rows


def exchange(blocks):
    return lax.all_to_all(blocks, "dp", split_axis=0, concat_axis=0, tiled=True)


def mix_heads(rows):
    count = lax.axis_size("expert")
    mine = lax.axis_index("expert")
    head = rows.shape[1] // count
    if head % 128 or count & (count - 1):
        return lax.all_to_all(rows, "expert", split_axis=1, concat_axis=1, tiled=True)
    pieces = []
    for k in range(count):
        piece = lax.dynamic_slice_in_dim(rows, (mine ^ k) * head, head, 1)
        pieces.append(lax.ppermute(piece, "expert", xor_pairs(count, k)) if k else piece)
    stacked = jnp.stack(pieces)
    return jnp.concatenate(
        [lax.dynamic_index_in_dim(stacked, mine ^ t, 0, False) for t in range(count)], axis=1
    )


def body(tokens, route_ids, router, norm_gain, w_in, w_out, cotangent):
    row_count = tokens.shape[0]
    model_width = tokens.shape[2]
    experts = lax.axis_size("dp")
    chips = experts // 2
    depth = 3 * row_count // experts
    weight_in = w_in[0, 0]
    weight_out = w_out[0, 0]
    hidden = weight_in.shape[1]
    router_row = router[0]
    gain_row = norm_gain[0]
    me = lax.axis_index("dp")
    far = list(range(chips // 2, chips))
    near = list(range(chips // 2))
    groups = [far[:1], near] + [[k] for k in far[1:]]

    route_rows = route_ids.reshape(row_count, 2)
    labels = lax.broadcasted_iota(jnp.int32, (row_count, 2, experts), 2)
    flat_hot = (route_rows[:, :, None] == labels).astype(jnp.int32).reshape(row_count * 2, experts)
    before = jnp.cumsum(flat_hot, axis=0, dtype=jnp.int32) - flat_hot
    slot_place = jnp.sum(before * flat_hot, axis=1, dtype=jnp.int32).reshape(row_count, 2)
    target = (route_rows ^ me) * depth + slot_place

    def placer_of(group):
        rows = []
        for k in group:
            slot = lax.broadcasted_iota(jnp.int32, (2 * depth, row_count), 0) + 2 * k * depth
            rows.append(jnp.logical_or(target[None, :, 0] == slot, target[None, :, 1] == slot))
        return jnp.concatenate(rows).astype(jnp.bfloat16) if len(rows) > 1 else rows[0].astype(jnp.bfloat16)

    placers = [placer_of(g) for g in groups]
    my_column = lax.broadcasted_iota(jnp.int32, (1, experts), 1) == me
    router_mine = jnp.sum(jnp.where(my_column, router_row.astype(jnp.float32), 0.0), axis=1)

    def dispatch(rows):
        arrived = []
        for group, placer in zip(groups, placers):
            slots = dot(placer, rows, ((1,), (0,))).astype(jnp.bfloat16)
            parts = [to_chip(slots[2 * depth * i : 2 * depth * (i + 1)], k) for i, k in enumerate(group)]
            mine = jnp.concatenate([p[:depth] for p in parts])
            others = jnp.concatenate([p[depth:] for p in parts])
            arrived.append(jnp.concatenate([mine, swap_cores(others)]))
        return arrived

    def give_back(group, rows):
        half = len(group) * depth
        others = swap_cores(rows[half:])
        parts = []
        for i, k in enumerate(group):
            pair = jnp.concatenate([rows[depth * i : depth * (i + 1)], others[depth * i : depth * (i + 1)]])
            parts.append(to_chip(pair, k))
        return jnp.concatenate(parts)

    def collect(start, parts):
        for place, rows in zip(placers[:-1], parts[:-1]):
            start = start + dot(place, rows, ((0,), (0,)))
        start = lax.optimization_barrier(start)
        return start + dot(placers[-1], parts[-1], ((0,), (0,)))

    mixed = mix_heads(tokens.reshape(row_count, model_width))
    kept, parts = [], []
    for group, rows in zip(groups, dispatch(mixed)):
        if parts:
            rows = after(rows, gated)
        logits = lax.optimization_barrier(dot(rows, router_row, ((1,), (0,))))
        gate = jax.nn.sigmoid(jnp.sum(jnp.where(my_column, logits, 0.0), axis=1, keepdims=True))
        pre_act = dot(rows, weight_in, ((1,), (0,)))
        act = gelu_tanh(pre_act).astype(jnp.bfloat16)
        out = dot(act, weight_out, ((1,), (0,)))
        kept.append((rows, gate, lax.optimization_barrier(pre_act), act, out.astype(jnp.bfloat16)))
        gated = (gate * out).astype(jnp.bfloat16)
        parts.append(give_back(group, gated))
    residual = collect(mixed.astype(jnp.float32), parts)
    row_mean = jnp.mean(residual, axis=1, keepdims=True)
    centered = residual - row_mean
    row_var = jnp.mean(centered * centered, axis=1, keepdims=True)
    inv_std = lax.rsqrt(row_var + norm_eps)
    normed = centered * inv_std
    normed_out = (normed * gain_row[None, :]).astype(jnp.bfloat16)
    cot_f = cotangent.reshape(row_count, model_width).astype(jnp.float32)
    grad_gain = jnp.sum(cot_f * normed, axis=0)
    grad_normed = cot_f * gain_row[None, :]
    grad_resid = inv_std * (
        grad_normed
        - jnp.mean(grad_normed, axis=1, keepdims=True)
        - normed * jnp.mean(grad_normed * normed, axis=1, keepdims=True)
    )

    slopes = []
    for saved in kept:
        slopes.append(lax.optimization_barrier(gelu_slope(saved[2])))
    router_parts = []
    parts, pre_grads, out_grads = [], [], []
    arrived = dispatch(grad_resid.astype(jnp.bfloat16))
    for g, (group, grads, saved) in enumerate(zip(groups, arrived, kept)):
        if parts:
            grads = after(grads, back)
        rows, gate, pre_act, act, result = saved
        grads_f = grads.astype(jnp.float32)
        grad_out = (gate * grads_f).astype(jnp.bfloat16)
        grad_gate = jnp.sum(grads_f * result.astype(jnp.float32), axis=1, keepdims=True)
        grad_logit = grad_gate * gate * (1.0 - gate)
        grad_act = dot(grad_out, weight_out, ((1,), (1,)))
        grad_pre = (grad_act * slopes[g]).astype(jnp.bfloat16)
        grad_input = dot(grad_pre, weight_in, ((1,), (1,))) + grad_logit * router_mine[None, :]
        back = grad_input.astype(jnp.bfloat16)
        parts.append(give_back(group, back))
        part = jnp.sum(rows.astype(jnp.float32) * grad_logit, axis=0)
        router_parts.append(lax.optimization_barrier(part))
        pre_grads.append(grad_pre)
        out_grads.append(grad_out)
    grad_mixed = collect(grad_resid, parts)
    grad_tokens = mix_heads(grad_mixed.astype(jnp.bfloat16))

    all_rows = jnp.concatenate([s[0] for s in kept])
    all_act = jnp.concatenate([s[3] for s in kept])
    lanes = 128
    small = jnp.stack([sum(router_parts), grad_gain]).reshape(1, 2 * model_width // lanes, lanes)
    small = exchange(jnp.broadcast_to(small, (experts,) + small.shape[1:]))
    small = small.reshape(experts, 2, model_width)
    grad_w_out = dot(all_act, jnp.concatenate(out_grads), ((0,), (0,))).astype(jnp.bfloat16)
    grad_w_in = dot(all_rows, jnp.concatenate(pre_grads), ((0,), (0,))).astype(jnp.bfloat16)
    return (
        normed_out.reshape(row_count, 1, model_width),
        grad_tokens.reshape(row_count, 1, model_width),
        small[:, 0].T.reshape(1, model_width, experts),
        jnp.sum(small[:, 1], axis=0).reshape(1, model_width),
        grad_w_in.reshape(1, 1, model_width, hidden),
        grad_w_out.reshape(1, 1, hidden, model_width),
    )


def solution(mesh):
    return jax.shard_map(
        body,
        mesh=mesh,
        in_specs=(
            P("dp", "expert", None),
            P("expert", "dp", None),
            P("expert", None, None),
            P("expert", None),
            P("expert", "dp", None, None),
            P("expert", "dp", None, None),
            P("dp", "expert", None),
        ),
        out_specs=(
            P("dp", "expert", None),
            P("dp", "expert", None),
            P("expert", None, None),
            P("expert", None),
            P("expert", "dp", None, None),
            P("expert", "dp", None, None),
        ),
        check_vma=False,
    )
```

```python
import jax
import jax.numpy as jnp
from jax import lax
from jax.sharding import PartitionSpec as P


gelu_coef = 0.7978845608028654
cubic_coef = 0.044715
norm_eps = 1e-05


def gelu_tanh(value):
    inner = gelu_coef * (value + cubic_coef * value * value * value)
    return 0.5 * value * (1.0 + jnp.tanh(inner))


def gelu_slope(value):
    inner = gelu_coef * (value + cubic_coef * value * value * value)
    tangent = jnp.tanh(inner)
    return 0.5 * (1.0 + tangent) + 0.5 * value * (1.0 - tangent * tangent) * gelu_coef * (
        1.0 + 3.0 * cubic_coef * value * value
    )


def dot(a, b, dims):
    return lax.dot_general(a, b, (dims, ((), ())), preferred_element_type=jnp.float32)


def after(rows, *others):
    return lax.optimization_barrier((rows,) + others)[0]


def xor_pairs(size, k):
    return [(i, i ^ k) for i in range(size)]


def swap_cores(rows):
    return lax.ppermute(rows, "dp", xor_pairs(lax.axis_size("dp"), 1))


def to_chip(rows, k):
    return lax.ppermute(rows, "dp", xor_pairs(lax.axis_size("dp"), 2 * k)) if k else rows


def exchange(blocks):
    return lax.all_to_all(blocks, "dp", split_axis=0, concat_axis=0, tiled=True)


def can_split(width):
    count = lax.axis_size("expert")
    return (width // count) % 128 == 0 and count & (count - 1) == 0


def blocks_of(rows, width):
    count = lax.axis_size("expert")
    head = width // count
    mine = lax.axis_index("expert")
    return [lax.dynamic_slice_in_dim(rows, (mine ^ k) * head, head, 1) for k in range(count)]


def in_order(pieces):
    count = lax.axis_size("expert")
    mine = lax.axis_index("expert")
    blocks = []
    for t in range(count):
        block = pieces[0]
        for k in range(1, count):
            block = jnp.where(mine ^ t == k, pieces[k], block)
        blocks.append(block)
    return jnp.concatenate(blocks, axis=1)


def cut(rows, width):
    head = width // lax.axis_size("expert")
    return [rows[:, i : i + head] for i in range(0, rows.shape[1], head)]


def swap_heads(pieces):
    moved = []
    for k, piece in enumerate(pieces):
        pairs = xor_pairs(lax.axis_size("expert"), k)
        moved.append(lax.ppermute(piece, "expert", pairs) if k else piece)
    return moved


def mix_heads(rows):
    if not can_split(rows.shape[1]):
        return lax.all_to_all(rows, "expert", split_axis=1, concat_axis=1, tiled=True)
    return in_order(swap_heads(blocks_of(rows, rows.shape[1])))


def body(tokens, route_ids, router, norm_gain, w_in, w_out, cotangent):
    row_count = tokens.shape[0]
    model_width = tokens.shape[2]
    experts = lax.axis_size("dp")
    chips = experts // 2
    depth = 3 * row_count // experts
    weight_in = w_in[0, 0]
    weight_out = w_out[0, 0]
    hidden = weight_in.shape[1]
    router_row = router[0]
    gain_row = norm_gain[0]
    me = lax.axis_index("dp")
    far = list(range(chips // 2, chips))
    near = list(range(chips // 2))
    groups = [far[:1], near] + [[k] for k in far[1:]]

    route_rows = route_ids.reshape(row_count, 2)
    labels = lax.broadcasted_iota(jnp.int32, (row_count, 2, experts), 2)
    flat_hot = (route_rows[:, :, None] == labels).astype(jnp.int32).reshape(row_count * 2, experts)
    before = jnp.cumsum(flat_hot, axis=0, dtype=jnp.int32) - flat_hot
    slot_place = jnp.sum(before * flat_hot, axis=1, dtype=jnp.int32).reshape(row_count, 2)
    target = (route_rows ^ me) * depth + slot_place

    def placer_of(group):
        rows = []
        for k in group:
            slot = lax.broadcasted_iota(jnp.int32, (2 * depth, row_count), 0) + 2 * k * depth
            rows.append(jnp.logical_or(target[None, :, 0] == slot, target[None, :, 1] == slot))
        return jnp.concatenate(rows).astype(jnp.bfloat16) if len(rows) > 1 else rows[0].astype(jnp.bfloat16)

    placers = [placer_of(g) for g in groups]
    my_column = lax.broadcasted_iota(jnp.int32, (1, experts), 1) == me
    router_mine = jnp.sum(jnp.where(my_column, router_row.astype(jnp.float32), 0.0), axis=1)

    def slots_of(placer, rows):
        return dot(placer, rows, ((1,), (0,))).astype(jnp.bfloat16)

    def dispatch(rows, pieces=None):
        arrived = []
        if pieces is not None:
            early = to_chip(slots_of(placers[0], pieces[0]), groups[0][0])
            rest = jnp.concatenate(pieces[1:], axis=1)
        for i, (group, placer) in enumerate(zip(groups, placers)):
            if pieces is not None and i == 0:
                late = to_chip(slots_of(placer, rest), group[0])
                whole = in_order([early] + cut(late, model_width))
                arrived.append(jnp.concatenate([whole[:depth], swap_cores(whole[depth:])]))
                continue
            slots = slots_of(placer, rows)
            parts = [to_chip(slots[2 * depth * i : 2 * depth * (i + 1)], k) for i, k in enumerate(group)]
            mine = jnp.concatenate([p[:depth] for p in parts])
            others = jnp.concatenate([p[depth:] for p in parts])
            arrived.append(jnp.concatenate([mine, swap_cores(others)]))
        return arrived

    def give_back(group, rows):
        half = len(group) * depth
        others = swap_cores(rows[half:])
        parts = []
        for i, k in enumerate(group):
            pair = jnp.concatenate([rows[depth * i : depth * (i + 1)], others[depth * i : depth * (i + 1)]])
            parts.append(to_chip(pair, k))
        return jnp.concatenate(parts)

    def partial_sum(start, parts):
        for place, rows in zip(placers[:-1], parts[:-1]):
            start = start + dot(place, rows, ((0,), (0,)))
        return lax.optimization_barrier(start)

    def collect(start, parts):
        start = partial_sum(start, parts)
        return start + dot(placers[-1], parts[-1], ((0,), (0,)))

    own_rows = tokens.reshape(row_count, model_width)
    split = can_split(model_width)
    if split:
        pieces = swap_heads(blocks_of(own_rows, model_width))
        mixed = in_order(pieces)
    else:
        pieces, mixed = None, mix_heads(own_rows)
    cot_f = cotangent.reshape(row_count, model_width).astype(jnp.float32)
    mean_grad = lax.optimization_barrier(jnp.mean(cot_f * gain_row[None, :], axis=1, keepdims=True))
    kept, parts = [], []
    for group, rows in zip(groups, dispatch(mixed, pieces)):
        if parts:
            rows = after(rows, gated)
        logits = lax.optimization_barrier(dot(rows, router_row, ((1,), (0,))))
        gate = jax.nn.sigmoid(jnp.sum(jnp.where(my_column, logits, 0.0), axis=1, keepdims=True))
        pre_act = dot(rows, weight_in, ((1,), (0,)))
        act = gelu_tanh(pre_act).astype(jnp.bfloat16)
        out = dot(act, weight_out, ((1,), (0,)))
        kept.append((rows, gate, lax.optimization_barrier(pre_act), act, out.astype(jnp.bfloat16)))
        gated = (gate * out).astype(jnp.bfloat16)
        parts.append(give_back(group, gated))
    residual = collect(mixed.astype(jnp.float32), parts)
    row_mean = jnp.mean(residual, axis=1, keepdims=True)
    centered = residual - row_mean
    row_var = jnp.mean(centered * centered, axis=1, keepdims=True)
    inv_std = lax.rsqrt(row_var + norm_eps)
    normed = centered * inv_std
    normed_out = (normed * gain_row[None, :]).astype(jnp.bfloat16)
    grad_gain = jnp.sum(cot_f * normed, axis=0)
    grad_normed = cot_f * gain_row[None, :]
    grad_resid = inv_std * (
        grad_normed
        - mean_grad
        - normed * jnp.mean(grad_normed * normed, axis=1, keepdims=True)
    )

    slopes = []
    for saved in kept:
        slopes.append(lax.optimization_barrier(gelu_slope(saved[2])))
    router_parts = []
    parts, pre_grads, out_grads = [], [], []
    arrived = dispatch(grad_resid.astype(jnp.bfloat16))
    for g, (group, grads, saved) in enumerate(zip(groups, arrived, kept)):
        if parts:
            grads = after(grads, back)
        rows, gate, pre_act, act, result = saved
        grads_f = grads.astype(jnp.float32)
        grad_out = (gate * grads_f).astype(jnp.bfloat16)
        grad_gate = jnp.sum(grads_f * result.astype(jnp.float32), axis=1, keepdims=True)
        grad_logit = grad_gate * gate * (1.0 - gate)
        grad_act = dot(grad_out, weight_out, ((1,), (1,)))
        grad_pre = (grad_act * slopes[g]).astype(jnp.bfloat16)
        grad_input = dot(grad_pre, weight_in, ((1,), (1,))) + grad_logit * router_mine[None, :]
        back = grad_input.astype(jnp.bfloat16)
        if split and g == len(groups) - 1:
            pair = jnp.concatenate([back[:depth], swap_cores(back[depth:])])
            own_block, *others = blocks_of(pair, model_width)
            parts.append(to_chip(jnp.concatenate(others, axis=1), group[0]))
            last_block = to_chip(own_block, group[0])
        else:
            parts.append(give_back(group, back))
        part = jnp.sum(rows.astype(jnp.float32) * grad_logit, axis=0)
        router_parts.append(lax.optimization_barrier(part))
        pre_grads.append(grad_pre)
        out_grads.append(grad_out)
    if split:
        start, *others = blocks_of(partial_sum(grad_resid, parts), model_width)
        main = jnp.concatenate(others, axis=1) + dot(placers[-1], parts[-1], ((0,), (0,)))
        main = main.astype(jnp.bfloat16)
        start = (start + dot(placers[-1], last_block, ((0,), (0,)))).astype(jnp.bfloat16)
        grad_tokens = in_order(swap_heads([start] + cut(main, model_width)))
    else:
        grad_tokens = mix_heads(collect(grad_resid, parts).astype(jnp.bfloat16))

    all_rows = jnp.concatenate([s[0] for s in kept])
    all_act = jnp.concatenate([s[3] for s in kept])
    lanes = 128
    small = jnp.stack([sum(router_parts), grad_gain]).reshape(1, 2 * model_width // lanes, lanes)
    small = exchange(jnp.broadcast_to(small, (experts,) + small.shape[1:]))
    small = small.reshape(experts, 2, model_width)
    grad_w_out = dot(all_act, jnp.concatenate(out_grads), ((0,), (0,))).astype(jnp.bfloat16)
    grad_w_in = dot(all_rows, jnp.concatenate(pre_grads), ((0,), (0,))).astype(jnp.bfloat16)
    return (
        normed_out.reshape(row_count, 1, model_width),
        grad_tokens.reshape(row_count, 1, model_width),
        small[:, 0].T.reshape(1, model_width, experts),
        jnp.sum(small[:, 1], axis=0).reshape(1, model_width),
        grad_w_in.reshape(1, 1, model_width, hidden),
        grad_w_out.reshape(1, 1, hidden, model_width),
    )


def solution(mesh):
    return jax.shard_map(
        body,
        mesh=mesh,
        in_specs=(
            P("dp", "expert", None),
            P("expert", "dp", None),
            P("expert", None, None),
            P("expert", None),
            P("expert", "dp", None, None),
            P("expert", "dp", None, None),
            P("dp", "expert", None),
        ),
        out_specs=(
            P("dp", "expert", None),
            P("dp", "expert", None),
            P("expert", None, None),
            P("expert", None),
            P("expert", "dp", None, None),
            P("expert", "dp", None, None),
        ),
        check_vma=False,
    )
```

```python
import jax
import jax.numpy as jnp
from jax import lax
from jax.sharding import PartitionSpec as P


gelu_coef = 0.7978845608028654
cubic_coef = 0.044715
norm_eps = 1e-05


def gelu_tanh(value):
    inner = gelu_coef * (value + cubic_coef * value * value * value)
    return 0.5 * value * (1.0 + jnp.tanh(inner))


def gelu_slope(value):
    inner = gelu_coef * (value + cubic_coef * value * value * value)
    tangent = jnp.tanh(inner)
    return 0.5 * (1.0 + tangent) + 0.5 * value * (1.0 - tangent * tangent) * gelu_coef * (
        1.0 + 3.0 * cubic_coef * value * value
    )


LINE_CHIPS = 4


def chip_pairs(pairs):
    return [(2 * a + core, 2 * b + core) for a, b in pairs for core in (0, 1)]


MIDDLE = chip_pairs([(1, 2), (2, 1)])
ENDS = chip_pairs([(0, 3), (3, 0)])
FOLD = chip_pairs([(2, 0), (1, 3), (3, 2), (0, 1)])


def move(rows, pairs):
    return lax.ppermute(rows, "dp", pairs)


def dot(a, b, dims):
    return lax.dot_general(a, b, (dims, ((), ())), preferred_element_type=jnp.float32)


def after(rows, *others):
    return lax.optimization_barrier((rows,) + others)[0]


def xor_pairs(size, k):
    return [(i, i ^ k) for i in range(size)]


def swap_cores(rows):
    return lax.ppermute(rows, "dp", xor_pairs(lax.axis_size("dp"), 1))


def to_chip(rows, k):
    return lax.ppermute(rows, "dp", xor_pairs(lax.axis_size("dp"), 2 * k)) if k else rows


def exchange(blocks):
    return lax.all_to_all(blocks, "dp", split_axis=0, concat_axis=0, tiled=True)


def can_split(width):
    count = lax.axis_size("expert")
    return (width // count) % 128 == 0 and count & (count - 1) == 0


def blocks_of(rows, width):
    count = lax.axis_size("expert")
    head = width // count
    mine = lax.axis_index("expert")
    return [lax.dynamic_slice_in_dim(rows, (mine ^ k) * head, head, 1) for k in range(count)]


def in_order(pieces):
    count = lax.axis_size("expert")
    mine = lax.axis_index("expert")
    blocks = []
    for t in range(count):
        block = pieces[0]
        for k in range(1, count):
            block = jnp.where(mine ^ t == k, pieces[k], block)
        blocks.append(block)
    return jnp.concatenate(blocks, axis=1)


def cut(rows, width):
    head = width // lax.axis_size("expert")
    return [rows[:, i : i + head] for i in range(0, rows.shape[1], head)]


def swap_heads(pieces):
    moved = []
    for k, piece in enumerate(pieces):
        pairs = xor_pairs(lax.axis_size("expert"), k)
        moved.append(lax.ppermute(piece, "expert", pairs) if k else piece)
    return moved


def mix_heads(rows):
    if not can_split(rows.shape[1]):
        return lax.all_to_all(rows, "expert", split_axis=1, concat_axis=1, tiled=True)
    return in_order(swap_heads(blocks_of(rows, rows.shape[1])))


def body(tokens, route_ids, router, norm_gain, w_in, w_out, cotangent):
    row_count = tokens.shape[0]
    model_width = tokens.shape[2]
    experts = lax.axis_size("dp")
    chips = experts // 2
    depth = 3 * row_count // experts
    weight_in = w_in[0, 0]
    weight_out = w_out[0, 0]
    hidden = weight_in.shape[1]
    router_row = router[0]
    gain_row = norm_gain[0]
    me = lax.axis_index("dp")
    far = list(range(chips // 2, chips))
    near = list(range(chips // 2))
    groups = [far[:1], near] + [[k] for k in far[1:]]

    route_rows = route_ids.reshape(row_count, 2)
    labels = lax.broadcasted_iota(jnp.int32, (row_count, 2, experts), 2)
    flat_hot = (route_rows[:, :, None] == labels).astype(jnp.int32).reshape(row_count * 2, experts)
    before = jnp.cumsum(flat_hot, axis=0, dtype=jnp.int32) - flat_hot
    slot_place = jnp.sum(before * flat_hot, axis=1, dtype=jnp.int32).reshape(row_count, 2)
    target = (route_rows ^ me) * depth + slot_place

    def placer_of(group):
        rows = []
        for k in group:
            slot = lax.broadcasted_iota(jnp.int32, (2 * depth, row_count), 0) + 2 * k * depth
            rows.append(jnp.logical_or(target[None, :, 0] == slot, target[None, :, 1] == slot))
        return jnp.concatenate(rows).astype(jnp.bfloat16) if len(rows) > 1 else rows[0].astype(jnp.bfloat16)

    placers = [placer_of(g) for g in groups]
    split = can_split(model_width)
    line = split and chips == LINE_CHIPS
    if line:
        inner = jnp.logical_or(me // 2 == 1, me // 2 == 2)
        far_target = move(target.T, MIDDLE)
        slot = lax.broadcasted_iota(jnp.int32, (2 * depth, row_count), 0)
        place_far = []
        for k in (3, 2):
            at = slot + 2 * k * depth
            place_far.append(jnp.logical_or(far_target[0][None, :] == at, far_target[1][None, :] == at))
        place_far = jnp.concatenate(place_far).astype(jnp.bfloat16)
        home = [jnp.where(inner, jnp.zeros_like(placers[0]), placers[0])] + placers[1:]
    else:
        home = placers
    my_column = lax.broadcasted_iota(jnp.int32, (1, experts), 1) == me
    router_mine = jnp.sum(jnp.where(my_column, router_row.astype(jnp.float32), 0.0), axis=1)

    def slots_of(placer, rows):
        return dot(placer, rows, ((1,), (0,))).astype(jnp.bfloat16)

    def dispatch(rows, pieces=None):
        arrived = []
        if pieces is not None:
            early = to_chip(slots_of(placers[0], pieces[0]), groups[0][0])
            rest = jnp.concatenate(pieces[1:], axis=1)
        for i, (group, placer) in enumerate(zip(groups, placers)):
            if pieces is not None and i == 0:
                late = to_chip(slots_of(placer, rest), group[0])
                whole = in_order([early] + cut(late, model_width))
                arrived.append(jnp.concatenate([whole[:depth], swap_cores(whole[depth:])]))
                continue
            slots = slots_of(placer, rows)
            parts = [to_chip(slots[2 * depth * i : 2 * depth * (i + 1)], k) for i, k in enumerate(group)]
            mine = jnp.concatenate([p[:depth] for p in parts])
            others = jnp.concatenate([p[depth:] for p in parts])
            arrived.append(jnp.concatenate([mine, swap_cores(others)]))
        return arrived

    def paired(rows):
        return jnp.concatenate([rows[:depth], swap_cores(rows[depth:])])

    def far_sum(pair, passed):
        return dot(place_far, jnp.concatenate([pair, passed]), ((0,), (0,))).astype(jnp.bfloat16)

    def give_back(group, rows):
        if line and group == groups[0]:
            return move(paired(rows), FOLD)
        half = len(group) * depth
        others = swap_cores(rows[half:])
        parts = []
        for i, k in enumerate(group):
            pair = jnp.concatenate([rows[depth * i : depth * (i + 1)], others[depth * i : depth * (i + 1)]])
            parts.append(to_chip(pair, k))
        return jnp.concatenate(parts)

    def partial_sum(start, parts):
        for place, rows in zip(home[:-1], parts[:-1]):
            start = start + dot(place, rows, ((0,), (0,)))
        return lax.optimization_barrier(start)

    def collect(start, parts):
        start = partial_sum(start, parts)
        return start + dot(placers[-1], parts[-1], ((0,), (0,)))

    own_rows = tokens.reshape(row_count, model_width)
    if split:
        pieces = swap_heads(blocks_of(own_rows, model_width))
        mixed = in_order(pieces)
    else:
        pieces, mixed = None, mix_heads(own_rows)
    cot_f = cotangent.reshape(row_count, model_width).astype(jnp.float32)
    mean_grad = lax.optimization_barrier(jnp.mean(cot_f * gain_row[None, :], axis=1, keepdims=True))
    kept, parts = [], []
    for g, (group, rows) in enumerate(zip(groups, dispatch(mixed, pieces))):
        if parts:
            rows = after(rows, gated)
        logits = lax.optimization_barrier(dot(rows, router_row, ((1,), (0,))))
        gate = jax.nn.sigmoid(jnp.sum(jnp.where(my_column, logits, 0.0), axis=1, keepdims=True))
        pre_act = dot(rows, weight_in, ((1,), (0,)))
        act = gelu_tanh(pre_act).astype(jnp.bfloat16)
        out = dot(act, weight_out, ((1,), (0,)))
        kept.append((rows, gate, lax.optimization_barrier(pre_act), act, out.astype(jnp.bfloat16)))
        gated = (gate * out).astype(jnp.bfloat16)
        if line and g == len(groups) - 1:
            pair = paired(gated)
            parts.append(move(pair, ENDS))
            crossed = move(far_sum(pair, parts[0]), MIDDLE)
        else:
            parts.append(give_back(group, gated))
    residual = collect(mixed.astype(jnp.float32), parts)
    if line:
        residual = residual + crossed.astype(jnp.float32)
    row_mean = jnp.mean(residual, axis=1, keepdims=True)
    centered = residual - row_mean
    row_var = jnp.mean(centered * centered, axis=1, keepdims=True)
    inv_std = lax.rsqrt(row_var + norm_eps)
    normed = centered * inv_std
    normed_out = (normed * gain_row[None, :]).astype(jnp.bfloat16)
    grad_gain = jnp.sum(cot_f * normed, axis=0)
    grad_normed = cot_f * gain_row[None, :]
    grad_resid = inv_std * (
        grad_normed
        - mean_grad
        - normed * jnp.mean(grad_normed * normed, axis=1, keepdims=True)
    )

    slopes = []
    for saved in kept:
        slopes.append(lax.optimization_barrier(gelu_slope(saved[2])))
    router_parts = []
    parts, pre_grads, out_grads = [], [], []
    arrived = dispatch(grad_resid.astype(jnp.bfloat16))
    for g, (group, grads, saved) in enumerate(zip(groups, arrived, kept)):
        if parts:
            grads = after(grads, back)
        rows, gate, pre_act, act, result = saved
        grads_f = grads.astype(jnp.float32)
        grad_out = (gate * grads_f).astype(jnp.bfloat16)
        grad_gate = jnp.sum(grads_f * result.astype(jnp.float32), axis=1, keepdims=True)
        grad_logit = grad_gate * gate * (1.0 - gate)
        grad_act = dot(grad_out, weight_out, ((1,), (1,)))
        grad_pre = (grad_act * slopes[g]).astype(jnp.bfloat16)
        grad_input = dot(grad_pre, weight_in, ((1,), (1,))) + grad_logit * router_mine[None, :]
        back = grad_input.astype(jnp.bfloat16)
        if split and g == len(groups) - 1:
            pair = paired(back)
            own_block, *others = blocks_of(pair, model_width)
            others = jnp.concatenate(others, axis=1)
            if line:
                parts.append(move(others, ENDS))
                own_sum, *other_sums = blocks_of(far_sum(pair, parts[0]), model_width)
                crossed = move(jnp.concatenate(other_sums, axis=1), MIDDLE)
                last_block = move(own_block, ENDS)
                last_crossed = move(own_sum, MIDDLE)
            else:
                parts.append(to_chip(others, group[0]))
                last_block = to_chip(own_block, group[0])
        else:
            parts.append(give_back(group, back))
        part = jnp.sum(rows.astype(jnp.float32) * grad_logit, axis=0)
        router_parts.append(lax.optimization_barrier(part))
        pre_grads.append(grad_pre)
        out_grads.append(grad_out)
    if split:
        start, *others = blocks_of(partial_sum(grad_resid, parts), model_width)
        main = jnp.concatenate(others, axis=1) + dot(placers[-1], parts[-1], ((0,), (0,)))
        main = (main + crossed.astype(jnp.float32) if line else main).astype(jnp.bfloat16)
        last_block = after(last_block, main)
        start = start + dot(placers[-1], last_block, ((0,), (0,)))
        start = (start + last_crossed.astype(jnp.float32) if line else start).astype(jnp.bfloat16)
        grad_tokens = in_order(swap_heads([start] + cut(main, model_width)))
    else:
        grad_tokens = mix_heads(collect(grad_resid, parts).astype(jnp.bfloat16))

    all_rows = jnp.concatenate([s[0] for s in kept])
    all_act = jnp.concatenate([s[3] for s in kept])
    lanes = 128
    small = jnp.stack([sum(router_parts), grad_gain]).reshape(1, 2 * model_width // lanes, lanes)
    small = exchange(jnp.broadcast_to(small, (experts,) + small.shape[1:]))
    small = small.reshape(experts, 2, model_width)
    grad_w_out = dot(all_act, jnp.concatenate(out_grads), ((0,), (0,))).astype(jnp.bfloat16)
    grad_w_in = dot(all_rows, jnp.concatenate(pre_grads), ((0,), (0,))).astype(jnp.bfloat16)
    return (
        normed_out.reshape(row_count, 1, model_width),
        grad_tokens.reshape(row_count, 1, model_width),
        small[:, 0].T.reshape(1, model_width, experts),
        jnp.sum(small[:, 1], axis=0).reshape(1, model_width),
        grad_w_in.reshape(1, 1, model_width, hidden),
        grad_w_out.reshape(1, 1, hidden, model_width),
    )


def solution(mesh):
    return jax.shard_map(
        body,
        mesh=mesh,
        in_specs=(
            P("dp", "expert", None),
            P("expert", "dp", None),
            P("expert", None, None),
            P("expert", None),
            P("expert", "dp", None, None),
            P("expert", "dp", None, None),
            P("dp", "expert", None),
        ),
        out_specs=(
            P("dp", "expert", None),
            P("dp", "expert", None),
            P("expert", None, None),
            P("expert", None),
            P("expert", "dp", None, None),
            P("expert", "dp", None, None),
        ),
        check_vma=False,
    )
```

```python
import jax
import jax.numpy as jnp
from jax import lax
from jax.experimental import pallas as pl
from jax.experimental.pallas import tpu as pltpu
from jax.sharding import PartitionSpec as P


gelu_coef = 0.7978845608028654
cubic_coef = 0.044715
norm_eps = 1e-05


def gelu_tanh(value):
    inner = gelu_coef * (value + cubic_coef * value * value * value)
    return 0.5 * value * (1.0 + jnp.tanh(inner))


def gelu_slope(value):
    inner = gelu_coef * (value + cubic_coef * value * value * value)
    tangent = jnp.tanh(inner)
    return 0.5 * (1.0 + tangent) + 0.5 * value * (1.0 - tangent * tangent) * gelu_coef * (
        1.0 + 3.0 * cubic_coef * value * value
    )


LINE_CHIPS = 4


def chip_pairs(pairs):
    return [(2 * a + core, 2 * b + core) for a, b in pairs for core in (0, 1)]


MIDDLE = chip_pairs([(1, 2), (2, 1)])
ENDS = chip_pairs([(0, 3), (3, 0)])
FOLD = chip_pairs([(2, 0), (1, 3), (3, 2), (0, 1)])


def move(rows, pairs):
    return lax.ppermute(rows, "dp", pairs)


def dot(a, b, dims):
    return lax.dot_general(a, b, (dims, ((), ())), preferred_element_type=jnp.float32)


def after(rows, *others):
    return lax.optimization_barrier((rows,) + others)[0]


def xor_pairs(size, k):
    return [(i, i ^ k) for i in range(size)]


def swap_cores(rows):
    return lax.ppermute(rows, "dp", xor_pairs(lax.axis_size("dp"), 1))


def to_chip(rows, k):
    return lax.ppermute(rows, "dp", xor_pairs(lax.axis_size("dp"), 2 * k)) if k else rows


def exchange(blocks):
    return lax.all_to_all(blocks, "dp", split_axis=0, concat_axis=0, tiled=True)


def can_split(width):
    count = lax.axis_size("expert")
    return (width // count) % 128 == 0 and count & (count - 1) == 0


def blocks_of(rows, width):
    count = lax.axis_size("expert")
    head = width // count
    mine = lax.axis_index("expert")
    return [lax.dynamic_slice_in_dim(rows, (mine ^ k) * head, head, 1) for k in range(count)]


def in_order(pieces):
    count = lax.axis_size("expert")
    mine = lax.axis_index("expert")
    blocks = []
    for t in range(count):
        block = pieces[0]
        for k in range(1, count):
            block = jnp.where(mine ^ t == k, pieces[k], block)
        blocks.append(block)
    return jnp.concatenate(blocks, axis=1)


def place_kernel(mine_ref, *refs):
    pieces, out = refs[:-1], refs[-1]
    head = pieces[0].shape[1]
    for own in range(len(pieces)):

        @pl.when(mine_ref[0] == own)
        def _():
            for t in range(len(pieces)):
                out[:, t * head : (t + 1) * head] = pieces[own ^ t][...]


def placed(pieces):
    rows, head = pieces[0].shape
    mine = lax.axis_index("expert").astype(jnp.int32).reshape(1)
    return pl.pallas_call(
        place_kernel,
        out_shape=jax.ShapeDtypeStruct((rows, head * len(pieces)), pieces[0].dtype),
        in_specs=[pl.BlockSpec(memory_space=pltpu.SMEM)]
        + [pl.BlockSpec(memory_space=pltpu.VMEM)] * len(pieces),
        out_specs=pl.BlockSpec(memory_space=pltpu.VMEM),
        compiler_params=pltpu.CompilerParams(vmem_limit_bytes=4 * 1024 * 1024),
    )(mine, *pieces)


def cut(rows, width):
    head = width // lax.axis_size("expert")
    return [rows[:, i : i + head] for i in range(0, rows.shape[1], head)]


def swap_heads(pieces):
    moved = []
    for k, piece in enumerate(pieces):
        pairs = xor_pairs(lax.axis_size("expert"), k)
        moved.append(lax.ppermute(piece, "expert", pairs) if k else piece)
    return moved


def mix_heads(rows):
    if not can_split(rows.shape[1]):
        return lax.all_to_all(rows, "expert", split_axis=1, concat_axis=1, tiled=True)
    return in_order(swap_heads(blocks_of(rows, rows.shape[1])))


def body(tokens, route_ids, router, norm_gain, w_in, w_out, cotangent):
    row_count = tokens.shape[0]
    model_width = tokens.shape[2]
    experts = lax.axis_size("dp")
    chips = experts // 2
    depth = 3 * row_count // experts
    weight_in = w_in[0, 0]
    weight_out = w_out[0, 0]
    hidden = weight_in.shape[1]
    router_row = router[0]
    gain_row = norm_gain[0]
    me = lax.axis_index("dp")
    far = list(range(chips // 2, chips))
    near = list(range(chips // 2))
    groups = [far[:1], near] + [[k] for k in far[1:]]

    route_rows = route_ids.reshape(row_count, 2)
    labels = lax.broadcasted_iota(jnp.int32, (row_count, 2, experts), 2)
    flat_hot = (route_rows[:, :, None] == labels).astype(jnp.int32).reshape(row_count * 2, experts)
    before = jnp.cumsum(flat_hot, axis=0, dtype=jnp.int32) - flat_hot
    slot_place = jnp.sum(before * flat_hot, axis=1, dtype=jnp.int32).reshape(row_count, 2)
    target = (route_rows ^ me) * depth + slot_place

    def placer_of(group):
        rows = []
        for k in group:
            slot = lax.broadcasted_iota(jnp.int32, (2 * depth, row_count), 0) + 2 * k * depth
            rows.append(jnp.logical_or(target[None, :, 0] == slot, target[None, :, 1] == slot))
        return jnp.concatenate(rows).astype(jnp.bfloat16) if len(rows) > 1 else rows[0].astype(jnp.bfloat16)

    placers = [placer_of(g) for g in groups]
    split = can_split(model_width)
    line = split and chips == LINE_CHIPS
    if line:
        inner = jnp.logical_or(me // 2 == 1, me // 2 == 2)
        far_target = move(target.T, MIDDLE)
        slot = lax.broadcasted_iota(jnp.int32, (2 * depth, row_count), 0)
        place_far = []
        for k in (3, 2):
            at = slot + 2 * k * depth
            place_far.append(jnp.logical_or(far_target[0][None, :] == at, far_target[1][None, :] == at))
        place_far = jnp.concatenate(place_far).astype(jnp.bfloat16)
        home = [jnp.where(inner, jnp.zeros_like(placers[0]), placers[0])] + placers[1:]
    else:
        home = placers
    my_column = lax.broadcasted_iota(jnp.int32, (1, experts), 1) == me
    router_mine = jnp.sum(jnp.where(my_column, router_row.astype(jnp.float32), 0.0), axis=1)

    def slots_of(placer, rows):
        return dot(placer, rows, ((1,), (0,))).astype(jnp.bfloat16)

    def dispatch(rows, pieces=None):
        arrived = []
        if pieces is not None:
            early = to_chip(slots_of(placers[0], pieces[0]), groups[0][0])
            rest = jnp.concatenate(pieces[1:], axis=1)
        for i, (group, placer) in enumerate(zip(groups, placers)):
            if pieces is not None and i == 0:
                late = to_chip(slots_of(placer, rest), group[0])
                whole = in_order([early] + cut(late, model_width))
                arrived.append(jnp.concatenate([whole[:depth], swap_cores(whole[depth:])]))
                continue
            slots = slots_of(placer, rows)
            parts = [to_chip(slots[2 * depth * i : 2 * depth * (i + 1)], k) for i, k in enumerate(group)]
            mine = jnp.concatenate([p[:depth] for p in parts])
            others = jnp.concatenate([p[depth:] for p in parts])
            arrived.append(jnp.concatenate([mine, swap_cores(others)]))
        return arrived

    def paired(rows):
        return jnp.concatenate([rows[:depth], swap_cores(rows[depth:])])

    def far_sum(pair, passed):
        both = jnp.concatenate([pair, passed])
        return dot(place_far, both, ((0,), (0,))).astype(jnp.bfloat16)

    def give_back(group, rows):
        if line and group == groups[0]:
            return move(paired(rows), FOLD)
        half = len(group) * depth
        others = swap_cores(rows[half:])
        parts = []
        for i, k in enumerate(group):
            pair = jnp.concatenate([rows[depth * i : depth * (i + 1)], others[depth * i : depth * (i + 1)]])
            parts.append(to_chip(pair, k))
        return jnp.concatenate(parts)

    def partial_sum(start, parts):
        for place, rows in zip(home[:-1], parts[:-1]):
            start = start + dot(place, rows, ((0,), (0,)))
        return lax.optimization_barrier(start)

    def collect(start, parts):
        start = partial_sum(start, parts)
        return start + dot(placers[-1], parts[-1], ((0,), (0,)))

    own_rows = tokens.reshape(row_count, model_width)
    if split:
        pieces = swap_heads(blocks_of(own_rows, model_width))
        mixed = in_order(pieces)
    else:
        pieces, mixed = None, mix_heads(own_rows)
    cot_f = cotangent.reshape(row_count, model_width).astype(jnp.float32)
    mean_grad = lax.optimization_barrier(jnp.mean(cot_f * gain_row[None, :], axis=1, keepdims=True))
    kept, parts = [], []
    for g, (group, rows) in enumerate(zip(groups, dispatch(mixed, pieces))):
        if parts:
            rows = after(rows, gated)
        logits = lax.optimization_barrier(dot(rows, router_row, ((1,), (0,))))
        gate = jax.nn.sigmoid(jnp.sum(jnp.where(my_column, logits, 0.0), axis=1, keepdims=True))
        pre_act = dot(rows, weight_in, ((1,), (0,)))
        act = gelu_tanh(pre_act).astype(jnp.bfloat16)
        out = dot(act, weight_out, ((1,), (0,)))
        kept.append((rows, gate, lax.optimization_barrier(pre_act), act, out.astype(jnp.bfloat16)))
        gated = (gate * out).astype(jnp.bfloat16)
        if line and g == len(groups) - 1:
            pair = paired(gated)
            parts.append(move(pair, ENDS))
            crossed = move(far_sum(pair, parts[0]), MIDDLE)
        else:
            parts.append(give_back(group, gated))
    residual = collect(mixed.astype(jnp.float32), parts)
    if line:
        residual = residual + crossed.astype(jnp.float32)
    row_mean = jnp.mean(residual, axis=1, keepdims=True)
    centered = residual - row_mean
    row_var = jnp.mean(centered * centered, axis=1, keepdims=True)
    inv_std = lax.rsqrt(row_var + norm_eps)
    normed = centered * inv_std
    normed_out = (normed * gain_row[None, :]).astype(jnp.bfloat16)
    grad_gain = jnp.sum(cot_f * normed, axis=0)
    grad_normed = cot_f * gain_row[None, :]
    grad_resid = inv_std * (
        grad_normed
        - mean_grad
        - normed * jnp.mean(grad_normed * normed, axis=1, keepdims=True)
    )

    slopes = []
    for saved in kept:
        slopes.append(lax.optimization_barrier(gelu_slope(saved[2])))
    router_parts = []
    parts, pre_grads, out_grads = [], [], []
    arrived = dispatch(grad_resid.astype(jnp.bfloat16))
    for g, (group, grads, saved) in enumerate(zip(groups, arrived, kept)):
        if parts:
            grads = after(grads, back)
        rows, gate, pre_act, act, result = saved
        grads_f = grads.astype(jnp.float32)
        grad_out = (gate * grads_f).astype(jnp.bfloat16)
        grad_gate = jnp.sum(grads_f * result.astype(jnp.float32), axis=1, keepdims=True)
        grad_logit = grad_gate * gate * (1.0 - gate)
        grad_act = dot(grad_out, weight_out, ((1,), (1,)))
        grad_pre = (grad_act * slopes[g]).astype(jnp.bfloat16)
        grad_input = dot(grad_pre, weight_in, ((1,), (1,))) + grad_logit * router_mine[None, :]
        back = grad_input.astype(jnp.bfloat16)
        if split and g == len(groups) - 1:
            pair = paired(back)
            own_block, *others = blocks_of(pair, model_width)
            others = jnp.concatenate(others, axis=1)
            if line:
                parts.append(move(others, ENDS))
                own_sum, *other_sums = blocks_of(far_sum(pair, parts[0]), model_width)
                crossed = move(jnp.concatenate(other_sums, axis=1), MIDDLE)
                last_block = move(own_block, ENDS)
                last_crossed = move(own_sum, MIDDLE)
            else:
                parts.append(to_chip(others, group[0]))
                last_block = to_chip(own_block, group[0])
        else:
            parts.append(give_back(group, back))
        part = jnp.sum(rows.astype(jnp.float32) * grad_logit, axis=0)
        router_parts.append(lax.optimization_barrier(part))
        pre_grads.append(grad_pre)
        out_grads.append(grad_out)
    if split:
        start, *others = blocks_of(partial_sum(grad_resid, parts), model_width)
        main = jnp.concatenate(others, axis=1) + dot(placers[-1], parts[-1], ((0,), (0,)))
        main = (main + crossed.astype(jnp.float32) if line else main).astype(jnp.bfloat16)
        last_block = after(last_block, main)
        start = start + dot(placers[-1], last_block, ((0,), (0,)))
        start = (start + last_crossed.astype(jnp.float32) if line else start).astype(jnp.bfloat16)
        grad_tokens = placed(swap_heads([start] + cut(main, model_width)))
    else:
        grad_tokens = mix_heads(collect(grad_resid, parts).astype(jnp.bfloat16))

    all_rows = jnp.concatenate([s[0] for s in kept])
    all_act = jnp.concatenate([s[3] for s in kept])
    lanes = 128
    small = jnp.stack([sum(router_parts), grad_gain]).reshape(1, 2 * model_width // lanes, lanes)
    small = exchange(jnp.broadcast_to(small, (experts,) + small.shape[1:]))
    small = small.reshape(experts, 2, model_width)
    grad_w_out = dot(all_act, jnp.concatenate(out_grads), ((0,), (0,))).astype(jnp.bfloat16)
    grad_w_in = dot(all_rows, jnp.concatenate(pre_grads), ((0,), (0,))).astype(jnp.bfloat16)
    return (
        normed_out.reshape(row_count, 1, model_width),
        grad_tokens.reshape(row_count, 1, model_width),
        small[:, 0].T.reshape(1, model_width, experts),
        jnp.sum(small[:, 1], axis=0).reshape(1, model_width),
        grad_w_in.reshape(1, 1, model_width, hidden),
        grad_w_out.reshape(1, 1, hidden, model_width),
    )


def solution(mesh):
    return jax.shard_map(
        body,
        mesh=mesh,
        in_specs=(
            P("dp", "expert", None),
            P("expert", "dp", None),
            P("expert", None, None),
            P("expert", None),
            P("expert", "dp", None, None),
            P("expert", "dp", None, None),
            P("dp", "expert", None),
        ),
        out_specs=(
            P("dp", "expert", None),
            P("dp", "expert", None),
            P("expert", None, None),
            P("expert", None),
            P("expert", "dp", None, None),
            P("expert", "dp", None, None),
        ),
        check_vma=False,
    )
```
